32 devices in a mesh: zero: 2 (over core), model: 16 (over z, y, x).
Axes of the slice: x: 2, y: 2, z: 4, core: 2. Of those that a mesh axis runs over, the one named last changes fastest.
Arguments:
- w_gate: float32 [5120, 13824], P('zero', 'model'), may hold values from -0.125 to 0.125
- first_gate: float32 [5120, 13824], P('zero', 'model'), may hold values from -0.078125 to 0.078125
- second_gate: float32 [5120, 13824], P('zero', 'model'), may hold values from -0.078125 to 0.078125
- w_up: float32 [5120, 13824], P('zero', 'model'), may hold values from -0.125 to 0.125
- first_up: float32 [5120, 13824], P('zero', 'model'), may hold values from -0.078125 to 0.078125
- second_up: float32 [5120, 13824], P('zero', 'model'), may hold values from -0.078125 to 0.078125
- norm_train: float32 [5120], P(('zero', 'model')), may hold values from 0.25 to 1.75
- norm_step: float32 [5120], P(('zero', 'model')), may hold values from -0.3 to 0.3
Outputs:
- ready_gate: bfloat16 [5120, 13824], P(None, 'model')
- ready_up: bfloat16 [5120, 13824], P(None, 'model')
- column_gate: float32 [13824], P('model')
- column_up: float32 [13824], P('model')
- serve_norm: bfloat16 [5120], replicated
- latest_gate: float32 [5120, 13824], P('zero', 'model')
- latest_up: float32 [5120, 13824], P('zero', 'model')
The draws below stay inside these ranges and needn't reach their ends.
All inputs are finite; a program needn't handle non-finite values. Where the reference program divides by a largest or mean magnitude, that divisor is 1e-20 or more.
Results may differ from the reference program's by a relative error of at most 0.001.
Values may be sent and summed in bfloat16 or wider, within the bound.
A program may use at most 192 MiB of HBM per device.

```python
import jax
import jax.numpy as jnp

D_MODEL = 5120
D_INNER = 13824


def strengthened(result, rng, source, target, parts, factor):
    def block_of(axis_at):
        return (jnp.arange(result.shape[axis_at]) // (result.shape[axis_at] // parts)).reshape((-1,) + (1,) * (result.ndim - 1 - axis_at))

    first = jax.random.permutation(rng, parts)[block_of(target)]
    second = (block_of(target) + parts // 2) % parts
    return jnp.where((block_of(source) == first) | (block_of(source) == second), factor * result, result)


def block_scale(stream_key, dims, split, smallest, largest):
    loudness, own = 1.0, jax.random.fold_in(stream_key, 6)
    for position, blocks in split:
        draws = jnp.exp(jax.random.uniform(jax.random.fold_in(own, position), (blocks,), jnp.float32, smallest / len(split), largest / len(split)))
        loudness = loudness * jnp.repeat(draws, dims[position] // blocks).reshape([-1 if axis == position else 1 for axis in range(len(dims))])
    return loudness


def scatter_about(stream_key, shape, spread, reach, pieces=(), dtype=jnp.bfloat16):
    loudness = block_scale(stream_key, shape, pieces, -0.22, 0.18) if pieces else 1.0
    values = jax.random.normal(stream_key, shape, jnp.float32) * spread * loudness
    return jnp.minimum(jnp.maximum(values, -reach), reach).astype(dtype)


def gaussian_with(key, shape, spread, most, split, heavy, kind=jnp.bfloat16):
    values = spread * jax.random.normal(key, shape, jnp.float32)
    if split:
        values = values * block_scale(key, shape, split, -0.22, 0.18)
    return jnp.clip(strengthened(values, jax.random.fold_in(key, 3), *heavy), -most, most).astype(kind)


def setup_inputs(seed: int = 0) -> dict:
    splits = jax.random.split(jax.random.key(seed), 9)
    w_gate = gaussian_with(splits[0], (D_MODEL, D_INNER), D_MODEL ** -0.5, 0.125, ((0, 2), (1, 16)), (0, 1, 16, 2.0), jnp.float32)
    first_gate = scatter_about(splits[1], (D_MODEL, D_INNER), D_MODEL ** -0.5, 0.078125, ((0, 2), (1, 16)), jnp.float32)
    second_gate = scatter_about(splits[2], (D_MODEL, D_INNER), D_MODEL ** -0.5, 0.078125, ((0, 2), (1, 16)), jnp.float32)
    w_up = gaussian_with(splits[3], (D_MODEL, D_INNER), D_MODEL ** -0.5, 0.125, ((0, 2), (1, 16)), (0, 1, 16, 2.0), jnp.float32)
    first_up = scatter_about(splits[4], (D_MODEL, D_INNER), D_MODEL ** -0.5, 0.078125, ((0, 2), (1, 16)), jnp.float32)
    second_up = scatter_about(splits[5], (D_MODEL, D_INNER), D_MODEL ** -0.5, 0.078125, ((0, 2), (1, 16)), jnp.float32)
    norm_train = jnp.clip(1.0 + 0.15 * jax.random.normal(splits[6], (D_MODEL,), jnp.float32), 0.25, 1.75)
    norm_step = jnp.clip(jax.random.uniform(splits[7], (D_MODEL,), jnp.float32, -0.3, 0.3) * block_scale(splits[7], (D_MODEL,), ((0, 32),), -0.4, 0.0), -0.3, 0.3)
    return dict(w_gate=w_gate, first_gate=first_gate, second_gate=second_gate, w_up=w_up, first_up=first_up, second_up=second_up, norm_train=norm_train, norm_step=norm_step)


learn_rate = 0.25
hold_rate = 0.8


def reference(w_gate, first_gate, second_gate, w_up, first_up, second_up, norm_train, norm_step):
    hold_gate = hold_rate * first_gate + second_gate
    latest_gate = w_gate - learn_rate * hold_gate
    hold_up = hold_rate * first_up + second_up
    latest_up = w_up - learn_rate * hold_up
    column_gate = jnp.max(jnp.abs(latest_gate), axis=0)
    ready_gate = (latest_gate / column_gate).astype(jnp.bfloat16)
    column_up = jnp.max(jnp.abs(latest_up), axis=0)
    ready_up = (latest_up / column_up).astype(jnp.bfloat16)
    serve_norm = (norm_train + norm_step).astype(jnp.bfloat16)
    return ready_gate, ready_up, column_gate, column_up, serve_norm, latest_gate, latest_up
```

```python
import functools

import jax
import jax.numpy as jnp
from jax import lax
from jax.experimental import pallas as pl
from jax.experimental.pallas import tpu as pltpu
from jax.sharding import PartitionSpec as P

learn_rate = 0.25
hold_rate = 0.8
LANES = 128
MESH = pl.DeviceIdType.MESH


def block_rows(rows, most):
    return max(k for k in range(16, most + 1, 16) if rows % k == 0)


def update_kernel(
    nz, nm, K, slots, lag,
    wg, fg, sg, wu, fu, su, norm_in,
    latest, ready, scale, norm_all,
    stage_f, stage_s, part, part_in,
    w_sem, f_sem, s_sem, part_send, part_recv, ready_send, ready_recv, norm_send, norm_recv,
):
    me = lax.axis_index("zero")
    col = lax.axis_index("model")
    n = nz * nm
    flat = me * nm + col
    rows, width = wg.shape
    nb = rows // K
    T = 2 * nb
    mine = pl.ds(pl.multiple_of(me * width, LANES), width)
    peers = [lax.rem(me + d, nz) for d in range(1, nz)]

    def copies(w, f, s, base, t):
        slot = lax.rem(t, slots)
        here = pl.ds(pl.multiple_of(base * K, 16), K)
        there = pl.ds(pl.multiple_of(t * K, 16), K)
        return (
            pltpu.make_async_copy(w.at[here], latest.at[there], w_sem.at[slot]),
            pltpu.make_async_copy(f.at[here], stage_f.at[slot], f_sem.at[slot]),
            pltpu.make_async_copy(s.at[here], stage_s.at[slot], s_sem.at[slot]),
        )

    def start(t):
        @pl.when(t < nb)
        def _():
            for c in copies(wg, fg, sg, t, t):
                c.start()

        @pl.when(t >= nb)
        def _():
            for c in copies(wu, fu, su, t - nb, t):
                c.start()

    def target(d):
        other = lax.rem(flat + d, n)
        return other // nm, lax.rem(other, nm)

    barrier = pltpu.get_barrier_semaphore()

    def greet(d, carry):
        pl.semaphore_signal(barrier, inc=1, device_id=target(d), device_id_type=MESH)
        return carry

    lax.fori_loop(1, n, greet, 0)
    for t in range(min(slots, T)):
        start(jnp.int32(t))
    norm_all[pl.ds(flat, 1)] = norm_in[...]
    pl.semaphore_wait(barrier, n - 1)

    def send_norm(d, carry):
        pltpu.make_async_remote_copy(
            src_ref=norm_in, dst_ref=norm_all.at[pl.ds(flat, 1)],
            send_sem=norm_send, recv_sem=norm_recv,
            device_id=target(d), device_id_type=MESH,
        ).start()
        return carry

    lax.fori_loop(1, n, send_norm, 0)

    def first_half(t):
        for c in copies(wg, fg, sg, 0, t):
            c.wait()
        slot = lax.rem(t, slots)
        for g in range(K // 8):
            r = pl.ds(pl.multiple_of(t * K + g * 8, 8), 8)
            hold = hold_rate * stage_f[slot, g * 8:(g + 1) * 8] + stage_s[slot, g * 8:(g + 1) * 8]
            new = latest[r, :] - learn_rate * hold
            latest[r, :] = new
            size = jnp.abs(new)
            most = size[:, :LANES]
            for i in range(1, width // LANES):
                most = jnp.maximum(most, size[:, i * LANES:(i + 1) * LANES])
            part[t, g * 8:(g + 1) * 8] = most

        @pl.when(t + slots < T)
        def _():
            start(t + slots)

        for i, peer in enumerate(peers):
            pltpu.make_async_remote_copy(
                src_ref=part.at[t], dst_ref=part_in.at[me, t],
                send_sem=part_send.at[i], recv_sem=part_recv.at[t, me],
                device_id={"zero": peer}, device_id_type=MESH,
            ).start()

    def second_half(u):
        most = part[u]
        for peer in peers:
            pltpu.make_async_copy(part_in.at[peer, u], part_in.at[peer, u], part_recv.at[u, peer]).wait()
            most = jnp.maximum(most, part_in[peer, u])
        most = jnp.max(most, axis=1, keepdims=True)
        there = pl.ds(pl.multiple_of(u * K, 16), K)
        scale[there, :] = jnp.broadcast_to(most, (K, LANES))
        inverse = 1.0 / most
        for g in range(K // 16):
            r = pl.ds(pl.multiple_of(u * K + g * 16, 16), 16)
            ready[r, mine] = (latest[r, :] * inverse[g * 16:(g + 1) * 16]).astype(jnp.bfloat16)
        for i, peer in enumerate(peers):
            pltpu.make_async_remote_copy(
                src_ref=ready.at[there, mine], dst_ref=ready.at[there, mine],
                send_sem=ready_send.at[i], recv_sem=ready_recv.at[me],
                device_id={"zero": peer}, device_id_type=MESH,
            ).start()

    def step(t, carry):
        first_half(t)

        @pl.when(t >= lag)
        def _():
            second_half(t - lag)

        return carry

    def last(u, carry):
        second_half(u)
        return carry

    lax.fori_loop(0, T, step, 0)
    lax.fori_loop(T - lag, T, last, 0)

    for i, peer in enumerate(peers):
        pltpu.make_async_copy(part, part, part_send.at[i]).wait()
        pltpu.make_async_copy(ready.at[:, mine], ready.at[:, mine], ready_send.at[i]).wait()
        theirs = pl.ds(pl.multiple_of(peer * width, LANES), width)
        pltpu.make_async_copy(ready.at[:, theirs], ready.at[:, theirs], ready_recv.at[peer]).wait()
    others = norm_all.at[pl.ds(0, n - 1)]
    pltpu.make_async_copy(others, others, norm_send).wait()
    pltpu.make_async_copy(others, others, norm_recv).wait()


def write_kernel(latest, ready, scale, ready_g, ready_u, latest_g, latest_u, column_g, column_u, sems):
    rows = latest_g.shape[0]
    copies = []
    for i, (src, dst) in enumerate(
        ((ready, ready_g), (ready, ready_u), (latest, latest_g), (latest, latest_u))
    ):
        c = pltpu.make_async_copy(src.at[pl.ds((i % 2) * rows, rows)], dst, sems.at[i])
        c.start()
        copies.append(c)
    for half, out in enumerate((column_g, column_u)):
        for first in range(0, rows, LANES):
            k = min(LANES, rows - first)
            tile = scale[half * rows + first:half * rows + first + k, :]
            diagonal = lax.broadcasted_iota(jnp.int32, (k, LANES), 0) == lax.broadcasted_iota(jnp.int32, (k, LANES), 1)
            line = jnp.sum(jnp.where(diagonal, tile, 0.0), axis=0, keepdims=True)
            out[:, first:first + k] = line[:, :k]
    for c in copies:
        c.wait()


def local(nz, nm, w_gate, first_gate, second_gate, w_up, first_up, second_up, norm_train, norm_step):
    n = nz * nm
    width, rows = w_gate.shape
    share = norm_train.shape[0]
    K = block_rows(rows, 48)
    T = 2 * rows // K
    slots = min(12, T)
    lag = 2
    norm_in = (norm_train + norm_step).reshape(1, 1, share)
    hbm = pl.BlockSpec(memory_space=pl.ANY)
    vmem = pl.BlockSpec(memory_space=pltpu.VMEM)
    latest, ready, scale, norm_all = pl.pallas_call(
        functools.partial(update_kernel, nz, nm, K, slots, lag),
        out_shape=(
            pltpu.VMEM((2 * rows, width), jnp.float32),
            pltpu.VMEM((2 * rows, nz * width), jnp.bfloat16),
            pltpu.VMEM((2 * rows, LANES), jnp.float32),
            pltpu.VMEM((n, 1, share), jnp.float32),
        ),
        in_specs=[hbm] * 6 + [vmem],
        out_specs=(vmem,) * 4,
        scratch_shapes=[
            pltpu.VMEM((slots, K, width), jnp.float32),
            pltpu.VMEM((slots, K, width), jnp.float32),
            pltpu.VMEM((T, K, LANES), jnp.float32),
            pltpu.VMEM((nz, T, K, LANES), jnp.float32),
            pltpu.SemaphoreType.DMA((slots,)),
            pltpu.SemaphoreType.DMA((slots,)),
            pltpu.SemaphoreType.DMA((slots,)),
            pltpu.SemaphoreType.DMA((max(nz - 1, 1),)),
            pltpu.SemaphoreType.DMA((T, nz)),
            pltpu.SemaphoreType.DMA((max(nz - 1, 1),)),
            pltpu.SemaphoreType.DMA((nz,)),
            pltpu.SemaphoreType.DMA,
            pltpu.SemaphoreType.DMA,
        ],
        compiler_params=pltpu.CompilerParams(
            collective_id=0, has_side_effects=True, vmem_limit_bytes=20 * 1024 * 1024
        ),
        name="update",
    )(w_gate.T, first_gate.T, second_gate.T, w_up.T, first_up.T, second_up.T, norm_in)
    ready_g, ready_u, latest_g, latest_u, column_g, column_u = pl.pallas_call(
        write_kernel,
        out_shape=(
            jax.ShapeDtypeStruct((rows, nz * width), jnp.bfloat16),
            jax.ShapeDtypeStruct((rows, nz * width), jnp.bfloat16),
            jax.ShapeDtypeStruct((rows, width), jnp.float32),
            jax.ShapeDtypeStruct((rows, width), jnp.float32),
            jax.ShapeDtypeStruct((1, rows), jnp.float32),
            jax.ShapeDtypeStruct((1, rows), jnp.float32),
        ),
        in_specs=[vmem] * 3,
        out_specs=(hbm,) * 4 + (vmem,) * 2,
        scratch_shapes=[pltpu.SemaphoreType.DMA((4,))],
        name="write",
    )(latest, ready, scale)
    serve_norm = norm_all.reshape(n * share).astype(jnp.bfloat16)
    return (
        ready_g.T, ready_u.T, column_g.reshape(rows), column_u.reshape(rows), serve_norm,
        latest_g.T, latest_u.T,
    )


def solution(mesh):
    whole, both = P("zero", "model"), P(("zero", "model"))
    return jax.shard_map(
        functools.partial(local, mesh.shape["zero"], mesh.shape["model"]),
        mesh=mesh,
        in_specs=(whole,) * 6 + (both,) * 2,
        out_specs=(
            P(None, "model"), P(None, "model"), P("model"), P("model"), P(), whole, whole,
        ),
        check_vma=False,
    )
```

```python
import functools

import jax
import jax.numpy as jnp
from jax import lax
from jax.experimental import pallas as pl
from jax.experimental.pallas import tpu as pltpu
from jax.sharding import PartitionSpec as P

learn_rate = 0.25
hold_rate = 0.8
LANES = 128
MESH = pl.DeviceIdType.MESH


def block_rows(rows, most):
    return max(k for k in range(16, most + 1, 16) if rows % k == 0)


def update_kernel(
    nz, nm, K, slots, lag,
    wg, fg, sg, wu, fu, su, norm_train, norm_step,
    ready_g, ready_u, column_g, column_u, latest_g, latest_u, serve_norm,
    stage_f, stage_s, part, part_in, scale, norm_all, norm_sum,
    w_sem, f_sem, s_sem, part_send, part_recv, ready_send, ready_recv, norm_send, norm_recv,
):
    me = lax.axis_index("zero")
    col = lax.axis_index("model")
    n = nz * nm
    flat = me * nm + col
    rows, width = wg.shape
    nb = rows // K
    T = 2 * nb
    mine = pl.ds(pl.multiple_of(me * width, LANES), width)
    peers = [lax.rem(me + d, nz) for d in range(1, nz)]
    gate = (wg, fg, sg, latest_g, ready_g, column_g, 0)
    up = (wu, fu, su, latest_u, ready_u, column_u, nb)

    def copies(side, t):
        w, f, s, latest, _, _, base = side
        slot = lax.rem(t, slots)
        here = pl.ds(pl.multiple_of((t - base) * K, 16), K)
        return (
            pltpu.make_async_copy(w.at[here], latest.at[here], w_sem.at[slot]),
            pltpu.make_async_copy(f.at[here], stage_f.at[slot], f_sem.at[slot]),
            pltpu.make_async_copy(s.at[here], stage_s.at[slot], s_sem.at[slot]),
        )

    def start(t):
        @pl.when(t < nb)
        def _():
            for c in copies(gate, t):
                c.start()

        @pl.when(t >= nb)
        def _():
            for c in copies(up, t):
                c.start()

    def target(d):
        other = lax.rem(flat + d, n)
        return other // nm, lax.rem(other, nm)

    barrier = pltpu.get_barrier_semaphore()

    for t in range(min(slots, T)):
        start(jnp.int32(t))

    def greet(d, carry):
        pl.semaphore_signal(barrier, inc=1, device_id=target(d), device_id_type=MESH)
        return carry

    lax.fori_loop(1, n, greet, 0)
    share = norm_train.shape[0]
    window = norm_all.shape[2]
    norm_all[flat] = jnp.zeros((1, window), jnp.float32)
    norm_all[flat, 0, 0:share] = norm_train[...] + norm_step[...]
    norm_all[flat] = pltpu.roll(norm_all[flat], lax.rem(flat * share, LANES), axis=1)
    pl.semaphore_wait(barrier, n - 1)

    def send_norm(d, carry):
        pltpu.make_async_remote_copy(
            src_ref=norm_all.at[flat], dst_ref=norm_all.at[flat],
            send_sem=norm_send, recv_sem=norm_recv,
            device_id=target(d), device_id_type=MESH,
        ).start()
        return carry

    lax.fori_loop(1, n, send_norm, 0)

    def first_half(side, t):
        latest, base = side[3], side[6]
        for c in copies(side, t):
            c.wait()
        slot = lax.rem(t, slots)
        for g in range(K // 8):
            r = pl.ds(pl.multiple_of((t - base) * K + g * 8, 8), 8)
            hold = hold_rate * stage_f[slot, g * 8:(g + 1) * 8] + stage_s[slot, g * 8:(g + 1) * 8]
            new = latest[r, :] - learn_rate * hold
            latest[r, :] = new
            size = jnp.abs(new)
            most = size[:, :LANES]
            for i in range(1, width // LANES):
                most = jnp.maximum(most, size[:, i * LANES:(i + 1) * LANES])
            part[t, g * 8:(g + 1) * 8] = most

        @pl.when(t + slots < T)
        def _():
            start(t + slots)

        for i, peer in enumerate(peers):
            pltpu.make_async_remote_copy(
                src_ref=part.at[t], dst_ref=part_in.at[me, t],
                send_sem=part_send.at[i], recv_sem=part_recv.at[t, me],
                device_id={"zero": peer}, device_id_type=MESH,
            ).start()

    def second_half(side, u):
        latest, ready, base = side[3], side[4], side[6]
        most = part[u]
        for peer in peers:
            pltpu.make_async_copy(part_in.at[peer, u], part_in.at[peer, u], part_recv.at[u, peer]).wait()
            most = jnp.maximum(most, part_in[peer, u])
        most = jnp.max(most, axis=1, keepdims=True)
        there = pl.ds(pl.multiple_of((u - base) * K, 16), K)
        scale[there, :] = jnp.broadcast_to(most, (K, LANES))
        inverse = 1.0 / most
        for g in range(K // 16):
            r = pl.ds(pl.multiple_of((u - base) * K + g * 16, 16), 16)
            ready[r, mine] = (latest[r, :] * inverse[g * 16:(g + 1) * 16]).astype(jnp.bfloat16)
        for i, peer in enumerate(peers):
            pltpu.make_async_remote_copy(
                src_ref=ready.at[there, mine], dst_ref=ready.at[there, mine],
                send_sem=ready_send.at[base // nb, i], recv_sem=ready_recv.at[base // nb, me],
                device_id={"zero": peer}, device_id_type=MESH,
            ).start()

    def columns(side):
        out = side[5]
        for first in range(0, rows, LANES):
            k = min(LANES, rows - first)
            tile = scale[first:first + k, :]
            diagonal = lax.broadcasted_iota(jnp.int32, (k, LANES), 0) == lax.broadcasted_iota(jnp.int32, (k, LANES), 1)
            line = jnp.sum(jnp.where(diagonal, tile, 0.0), axis=0)
            out[first:first + k] = line[:k]

    def run(low, high, ahead, behind):
        def step(t, carry):
            if ahead is not None:
                first_half(ahead, t)
            if behind is not None:
                second_half(behind, t - lag)
            return carry

        lax.fori_loop(low, high, step, 0)

    run(0, lag, gate, None)
    run(lag, nb, gate, gate)
    run(nb, nb + lag, up, gate)
    columns(gate)
    run(nb + lag, T, up, up)
    run(T, T + lag, None, up)
    columns(up)

    for i, peer in enumerate(peers):
        pltpu.make_async_copy(part, part, part_send.at[i]).wait()
        theirs = pl.ds(pl.multiple_of(peer * width, LANES), width)
        for half, ready in enumerate((ready_g, ready_u)):
            pltpu.make_async_copy(ready.at[:, mine], ready.at[:, mine], ready_send.at[half, i]).wait()
            pltpu.make_async_copy(ready.at[:, theirs], ready.at[:, theirs], ready_recv.at[half, peer]).wait()
    others = norm_all.at[pl.ds(0, n - 1)]
    pltpu.make_async_copy(others, others, norm_send).wait()
    pltpu.make_async_copy(others, others, norm_recv).wait()
    norm_sum[...] = jnp.zeros_like(norm_sum)
    for d in range(n):
        first = d * share // LANES * LANES
        norm_sum[:, first:first + window] += norm_all[d]
    serve_norm[...] = norm_sum[0, :n * share].astype(jnp.bfloat16)


def copy_kernel(*refs):
    sems = refs[8]
    copies = [pltpu.make_async_copy(refs[i], refs[4 + i], sems.at[i]) for i in range(4)]
    for c in copies:
        c.start()
    for c in copies:
        c.wait()


def local(nz, nm, w_gate, first_gate, second_gate, w_up, first_up, second_up, norm_train, norm_step):
    n = nz * nm
    width, rows = w_gate.shape
    share = norm_train.shape[0]
    K = block_rows(rows, 48)
    T = 2 * rows // K
    slots = min(8, T)
    lag = 2
    window = -(-(share + LANES - 1) // LANES) * LANES
    hbm = pl.BlockSpec(memory_space=pl.ANY)
    vmem = pl.BlockSpec(memory_space=pltpu.VMEM)
    ready_g, ready_u, column_g, column_u, latest_g, latest_u, serve_norm = pl.pallas_call(
        functools.partial(update_kernel, nz, nm, K, slots, lag),
        out_shape=(
            pltpu.VMEM((rows, nz * width), jnp.bfloat16),
            pltpu.VMEM((rows, nz * width), jnp.bfloat16),
            pltpu.VMEM((rows,), jnp.float32),
            pltpu.VMEM((rows,), jnp.float32),
            pltpu.VMEM((rows, width), jnp.float32),
            pltpu.VMEM((rows, width), jnp.float32),
            pltpu.VMEM((n * share,), jnp.bfloat16),
        ),
        in_specs=[hbm] * 6 + [vmem] * 2,
        out_specs=(vmem,) * 7,
        scratch_shapes=[
            pltpu.VMEM((slots, K, width), jnp.float32),
            pltpu.VMEM((slots, K, width), jnp.float32),
            pltpu.VMEM((T, K, LANES), jnp.float32),
            pltpu.VMEM((nz, T, K, LANES), jnp.float32),
            pltpu.VMEM((rows, LANES), jnp.float32),
            pltpu.VMEM((n, 1, window), jnp.float32),
            pltpu.VMEM((1, n * share + window), jnp.float32),
            pltpu.SemaphoreType.DMA((slots,)),
            pltpu.SemaphoreType.DMA((slots,)),
            pltpu.SemaphoreType.DMA((slots,)),
            pltpu.SemaphoreType.DMA((max(nz - 1, 1),)),
            pltpu.SemaphoreType.DMA((T, nz)),
            pltpu.SemaphoreType.DMA((2, max(nz - 1, 1))),
            pltpu.SemaphoreType.DMA((2, nz)),
            pltpu.SemaphoreType.DMA,
            pltpu.SemaphoreType.DMA,
        ],
        compiler_params=pltpu.CompilerParams(
            collective_id=0, has_side_effects=True, vmem_limit_bytes=12 * 1024 * 1024
        ),
        name="update",
    )(w_gate.T, first_gate.T, second_gate.T, w_up.T, first_up.T, second_up.T, norm_train, norm_step)
    ready_g, ready_u, latest_g, latest_u = pl.pallas_call(
        copy_kernel,
        out_shape=tuple(jax.ShapeDtypeStruct(x.shape, x.dtype) for x in (ready_g, ready_u, latest_g, latest_u)),
        in_specs=[hbm] * 4,
        out_specs=(hbm,) * 4,
        scratch_shapes=[pltpu.SemaphoreType.DMA((4,))],
        compiler_params=pltpu.CompilerParams(vmem_limit_bytes=1024 * 1024),
        name="write",
    )(ready_g, ready_u, latest_g, latest_u)
    return (ready_g.T, ready_u.T, column_g, column_u, serve_norm, latest_g.T, latest_u.T)


def solution(mesh):
    whole, both = P("zero", "model"), P(("zero", "model"))
    return jax.shard_map(
        functools.partial(local, mesh.shape["zero"], mesh.shape["model"]),
        mesh=mesh,
        in_specs=(whole,) * 6 + (both,) * 2,
        out_specs=(
            P(None, "model"), P(None, "model"), P("model"), P("model"), P(), whole, whole,
        ),
        check_vma=False,
    )
```

```python
import functools

import jax
import jax.numpy as jnp
from jax import lax
from jax.experimental import pallas as pl
from jax.experimental.pallas import tpu as pltpu
from jax.sharding import PartitionSpec as P

learn_rate = 0.25
hold_rate = 0.8
LANES = 128
MESH = pl.DeviceIdType.MESH


def block_rows(rows, most):
    return max(k for k in range(16, most + 1, 16) if rows % k == 0)


def update_kernel(
    nz, nm, K, slots, lag, quiet,
    wg, fg, sg, wu, fu, su, norm_train, norm_step,
    ready_g, ready_u, column_g, column_u, latest_g, latest_u, serve_norm,
    stage_f, stage_s, part, part_in, scale, norm_all, norm_sum, norm_a, norm_b,
    w_sem, f_sem, s_sem, part_send, part_recv, ready_send, ready_recv, norm_send, norm_recv, early_recv, norm_sem,
):
    me = lax.axis_index("zero")
    col = lax.axis_index("model")
    n = nz * nm
    flat = me * nm + col
    rows, width = wg.shape
    nb = rows // K
    T = 2 * nb
    mine = pl.ds(pl.multiple_of(me * width, LANES), width)
    peers = [lax.rem(me + d, nz) for d in range(1, nz)]
    gate = (wg, fg, sg, latest_g, ready_g, column_g, 0)
    up = (wu, fu, su, latest_u, ready_u, column_u, nb)

    def copies(side, t):
        w, f, s, latest, _, _, base = side
        slot = lax.rem(t, slots)
        here = pl.ds(pl.multiple_of((t - base) * K, 16), K)
        return (
            pltpu.make_async_copy(w.at[here], latest.at[here], w_sem.at[slot]),
            pltpu.make_async_copy(f.at[here], stage_f.at[slot], f_sem.at[slot]),
            pltpu.make_async_copy(s.at[here], stage_s.at[slot], s_sem.at[slot]),
        )

    def start(t):
        @pl.when(t < nb)
        def _():
            for c in copies(gate, t):
                c.start()

        @pl.when(t >= nb)
        def _():
            for c in copies(up, t):
                c.start()

    def target(d):
        other = lax.rem(flat + d, n)
        return other // nm, lax.rem(other, nm)

    barrier = pltpu.get_barrier_semaphore()

    norm_copies = (
        pltpu.make_async_copy(norm_train, norm_a, norm_sem.at[0]),
        pltpu.make_async_copy(norm_step, norm_b, norm_sem.at[1]),
    )
    for c in norm_copies:
        c.start()
    for t in range(min(slots, T)):
        start(jnp.int32(t))

    def greet(d, carry):
        pl.semaphore_signal(barrier, inc=1, device_id=target(d), device_id_type=MESH)
        return carry

    lax.fori_loop(1, n, greet, 0)
    share = norm_train.shape[0]
    window = norm_all.shape[2]
    norm_all[flat] = jnp.zeros((1, window), jnp.float32)

    def first_half(side, t):
        latest, base = side[3], side[6]
        for c in copies(side, t):
            c.wait()
        slot = lax.rem(t, slots)
        for g in range(K // 8):
            r = pl.ds(pl.multiple_of((t - base) * K + g * 8, 8), 8)
            hold = hold_rate * stage_f[slot, g * 8:(g + 1) * 8] + stage_s[slot, g * 8:(g + 1) * 8]
            new = latest[r, :] - learn_rate * hold
            latest[r, :] = new
            size = jnp.abs(new)
            most = size[:, :LANES]
            for i in range(1, width // LANES):
                most = jnp.maximum(most, size[:, i * LANES:(i + 1) * LANES])
            part[t, g * 8:(g + 1) * 8] = most

        @pl.when(t + slots < T)
        def _():
            start(t + slots)

    def second_half(side, u):
        latest, ready, base = side[3], side[4], side[6]
        most = part[u]
        for peer in peers:
            @pl.when(u >= quiet)
            def _():
                pltpu.make_async_copy(part_in.at[peer, u], part_in.at[peer, u], part_recv.at[u, peer]).wait()

            most = jnp.maximum(most, part_in[peer, u])
        most = jnp.max(most, axis=1, keepdims=True)
        there = pl.ds(pl.multiple_of((u - base) * K, 16), K)
        scale[pl.ds(pl.multiple_of(u * K, 16), K), :] = jnp.broadcast_to(most, (K, LANES))
        inverse = 1.0 / most
        for g in range(K // 16):
            r = pl.ds(pl.multiple_of((u - base) * K + g * 16, 16), 16)
            ready[r, mine] = (latest[r, :] * inverse[g * 16:(g + 1) * 16]).astype(jnp.bfloat16)
        for i, peer in enumerate(peers):
            pltpu.make_async_remote_copy(
                src_ref=ready.at[there, mine], dst_ref=ready.at[there, mine],
                send_sem=ready_send.at[base // nb, i], recv_sem=ready_recv.at[base // nb, me],
                device_id={"zero": peer}, device_id_type=MESH,
            ).start()

    def columns(side):
        out = side[5]
        for first in range(0, rows, LANES):
            k = min(LANES, rows - first)
            tile = scale[side[6] * K + first:side[6] * K + first + k, :]
            diagonal = lax.broadcasted_iota(jnp.int32, (k, LANES), 0) == lax.broadcasted_iota(jnp.int32, (k, LANES), 1)
            line = jnp.sum(jnp.where(diagonal, tile, 0.0), axis=0)
            out[first:first + k] = line[:k]

    def ahead(t):
        @pl.when(t < nb)
        def _():
            first_half(gate, t)

        @pl.when(t >= nb)
        def _():
            first_half(up, t)

    def behind(u):
        @pl.when(u < nb)
        def _():
            second_half(gate, u)

        @pl.when(u >= nb)
        def _():
            second_half(up, u)

    def send_part(t):
        for i, peer in enumerate(peers):
            pltpu.make_async_remote_copy(
                src_ref=part.at[t], dst_ref=part_in.at[me, t],
                send_sem=part_send.at[i], recv_sem=part_recv.at[t, me],
                device_id={"zero": peer}, device_id_type=MESH,
            ).start()

    def alone(t, carry):
        ahead(t)
        return carry

    def catch_up(i, carry):
        ahead(quiet + i)
        send_part(quiet + i)
        behind(2 * i)
        behind(2 * i + 1)
        return carry

    def steady(t, carry):
        ahead(t)
        send_part(t)
        behind(t - lag)
        return carry

    def last(u, carry):
        behind(u)
        return carry

    lax.fori_loop(0, quiet, alone, 0)
    for c in norm_copies:
        c.wait()
    norm_all[flat, 0, 0:share] = norm_a[...] + norm_b[...]
    norm_all[flat] = pltpu.roll(norm_all[flat], lax.rem(flat * share, LANES), axis=1)
    pl.semaphore_wait(barrier, n - 1)
    early = pl.ds(0, quiet)
    for i, peer in enumerate(peers):
        pltpu.make_async_remote_copy(
            src_ref=part.at[early], dst_ref=part_in.at[me, early],
            send_sem=part_send.at[i], recv_sem=early_recv.at[me],
            device_id={"zero": peer}, device_id_type=MESH,
        ).start()

    def send_norm(d, carry):
        pltpu.make_async_remote_copy(
            src_ref=norm_all.at[flat], dst_ref=norm_all.at[flat],
            send_sem=norm_send, recv_sem=norm_recv,
            device_id=target(d), device_id_type=MESH,
        ).start()
        return carry

    lax.fori_loop(1, n, send_norm, 0)
    for peer in peers:
        pltpu.make_async_copy(part_in.at[peer, early], part_in.at[peer, early], early_recv.at[peer]).wait()
    lax.fori_loop(0, quiet - lag, catch_up, 0)
    lax.fori_loop(2 * quiet - lag, T, steady, 0)
    columns(gate)
    others = norm_all.at[pl.ds(0, n - 1)]
    pltpu.make_async_copy(others, others, norm_send).wait()
    pltpu.make_async_copy(others, others, norm_recv).wait()
    norm_sum[...] = jnp.zeros_like(norm_sum)
    for d in range(n):
        first = d * share // LANES * LANES
        norm_sum[:, first:first + window] += norm_all[d]
    serve_norm[...] = norm_sum[0, :n * share].astype(jnp.bfloat16)
    lax.fori_loop(T - lag, T, last, 0)
    columns(up)

    for i, peer in enumerate(peers):
        pltpu.make_async_copy(part, part, part_send.at[i]).wait()
        theirs = pl.ds(pl.multiple_of(peer * width, LANES), width)
        for half, ready in enumerate((ready_g, ready_u)):
            pltpu.make_async_copy(ready.at[:, mine], ready.at[:, mine], ready_send.at[half, i]).wait()
            pltpu.make_async_copy(ready.at[:, theirs], ready.at[:, theirs], ready_recv.at[half, peer]).wait()


def copy_kernel(*refs):
    count = len(refs) // 2
    sems = refs[-1]
    copies = [pltpu.make_async_copy(refs[i], refs[count + i], sems.at[i]) for i in range(count)]
    for c in copies:
        c.start()
    for c in copies:
        c.wait()


def local(nz, nm, w_gate, first_gate, second_gate, w_up, first_up, second_up, norm_train, norm_step):
    n = nz * nm
    width, rows = w_gate.shape
    share = norm_train.shape[0]
    K = block_rows(rows, 48)
    T = 2 * rows // K
    slots = min(8, T)
    lag = 2
    quiet = max(lag, min(14, (T + lag) // 2))
    window = -(-(share + LANES - 1) // LANES) * LANES
    hbm = pl.BlockSpec(memory_space=pl.ANY)
    vmem = pl.BlockSpec(memory_space=pltpu.VMEM)
    ready_g, ready_u, column_g, column_u, latest_g, latest_u, serve_norm = pl.pallas_call(
        functools.partial(update_kernel, nz, nm, K, slots, lag, quiet),
        out_shape=(
            pltpu.VMEM((rows, nz * width), jnp.bfloat16),
            pltpu.VMEM((rows, nz * width), jnp.bfloat16),
            pltpu.VMEM((rows,), jnp.float32),
            pltpu.VMEM((rows,), jnp.float32),
            pltpu.VMEM((rows, width), jnp.float32),
            pltpu.VMEM((rows, width), jnp.float32),
            pltpu.VMEM((n * share,), jnp.bfloat16),
        ),
        in_specs=[hbm] * 6 + [pl.BlockSpec(memory_space=pltpu.HBM)] * 2,
        out_specs=(vmem,) * 7,
        scratch_shapes=[
            pltpu.VMEM((slots, K, width), jnp.float32),
            pltpu.VMEM((slots, K, width), jnp.float32),
            pltpu.VMEM((T, K, LANES), jnp.float32),
            pltpu.VMEM((nz, T, K, LANES), jnp.float32),
            pltpu.VMEM((2 * rows, LANES), jnp.float32),
            pltpu.VMEM((n, 1, window), jnp.float32),
            pltpu.VMEM((1, n * share + window), jnp.float32),
            pltpu.VMEM((share,), jnp.float32),
            pltpu.VMEM((share,), jnp.float32),
            pltpu.SemaphoreType.DMA((slots,)),
            pltpu.SemaphoreType.DMA((slots,)),
            pltpu.SemaphoreType.DMA((slots,)),
            pltpu.SemaphoreType.DMA((max(nz - 1, 1),)),
            pltpu.SemaphoreType.DMA((T, nz)),
            pltpu.SemaphoreType.DMA((2, max(nz - 1, 1))),
            pltpu.SemaphoreType.DMA((2, nz)),
            pltpu.SemaphoreType.DMA,
            pltpu.SemaphoreType.DMA,
            pltpu.SemaphoreType.DMA((nz,)),
            pltpu.SemaphoreType.DMA((2,)),
        ],
        compiler_params=pltpu.CompilerParams(
            collective_id=0, has_side_effects=True, vmem_limit_bytes=12 * 1024 * 1024
        ),
        name="update",
    )(w_gate.T, first_gate.T, second_gate.T, w_up.T, first_up.T, second_up.T, *(
        pltpu.with_memory_space_constraint(x, pltpu.HBM) for x in (norm_train, norm_step)
    ))
    results = (ready_g, ready_u, column_g, column_u, latest_g, latest_u, serve_norm)
    ready_g, ready_u, column_g, column_u, latest_g, latest_u, serve_norm = pl.pallas_call(
        copy_kernel,
        out_shape=tuple(jax.ShapeDtypeStruct(x.shape, x.dtype) for x in results),
        in_specs=[hbm] * 7,
        out_specs=(hbm,) * 7,
        scratch_shapes=[pltpu.SemaphoreType.DMA((7,))],
        compiler_params=pltpu.CompilerParams(vmem_limit_bytes=1024 * 1024),
        name="write",
    )(*results)
    return (ready_g.T, ready_u.T, column_g, column_u, serve_norm, latest_g.T, latest_u.T)


def solution(mesh):
    whole, both = P("zero", "model"), P(("zero", "model"))
    return jax.shard_map(
        functools.partial(local, mesh.shape["zero"], mesh.shape["model"]),
        mesh=mesh,
        in_specs=(whole,) * 6 + (both,) * 2,
        out_specs=(
            P(None, "model"), P(None, "model"), P("model"), P("model"), P(), whole, whole,
        ),
        check_vma=False,
    )
```

```python
import functools

import jax
import jax.numpy as jnp
from jax import lax
from jax.experimental import pallas as pl
from jax.experimental.pallas import tpu as pltpu
from jax.sharding import PartitionSpec as P

learn_rate = 0.25
hold_rate = 0.8
LANES = 128
MESH = pl.DeviceIdType.MESH


def block_rows(rows, most):
    return max(k for k in range(16, most + 1, 16) if rows % k == 0)


def update_kernel(
    nz, nm, K, slots, lag, quiet,
    wg, fg, sg, wu, fu, su, norm_train, norm_step,
    ready_g, ready_u, column_g, column_u, latest_g, latest_u, serve_norm,
    stage_f, stage_s, part, part_in, scale, norm_all, norm_sum, norm_a, norm_b,
    w_sem, f_sem, s_sem, part_send, part_recv, ready_send, ready_recv, norm_send, norm_recv, early_recv, norm_sem,
):
    me = lax.axis_index("zero")
    col = lax.axis_index("model")
    n = nz * nm
    flat = me * nm + col
    rows, width = wg.shape
    nb = rows // K
    T = 2 * nb
    mine = pl.ds(pl.multiple_of(me * width, LANES), width)
    peers = [lax.rem(me + d, nz) for d in range(1, nz)]
    gate = (wg, fg, sg, latest_g, ready_g, column_g, 0)
    up = (wu, fu, su, latest_u, ready_u, column_u, nb)

    def copies(side, t):
        w, f, s, latest, _, _, base = side
        slot = lax.rem(t, slots)
        here = pl.ds(pl.multiple_of((t - base) * K, 16), K)
        return (
            pltpu.make_async_copy(w.at[here], latest.at[here], w_sem.at[slot]),
            pltpu.make_async_copy(f.at[here], stage_f.at[slot], f_sem.at[slot]),
            pltpu.make_async_copy(s.at[here], stage_s.at[slot], s_sem.at[slot]),
        )

    def start(t):
        @pl.when(t < nb)
        def _():
            for c in copies(gate, t):
                c.start()

        @pl.when(t >= nb)
        def _():
            for c in copies(up, t):
                c.start()

    def target(d):
        other = lax.rem(flat + d, n)
        return other // nm, lax.rem(other, nm)

    barrier = pltpu.get_barrier_semaphore()

    norm_copies = (
        pltpu.make_async_copy(norm_train, norm_a, norm_sem.at[0]),
        pltpu.make_async_copy(norm_step, norm_b, norm_sem.at[1]),
    )
    for c in norm_copies:
        c.start()
    for t in range(min(slots, T)):
        start(jnp.int32(t))

    def greet(d, carry):
        pl.semaphore_signal(barrier, inc=1, device_id=target(d), device_id_type=MESH)
        return carry

    lax.fori_loop(1, n, greet, 0)
    share = norm_train.shape[0]
    window = norm_all.shape[2]
    norm_all[flat] = jnp.zeros((1, window), jnp.float32)

    def first_half(side, t):
        latest, base = side[3], side[6]
        for c in copies(side, t):
            c.wait()
        slot = lax.rem(t, slots)
        for g in range(K // 8):
            r = pl.ds(pl.multiple_of((t - base) * K + g * 8, 8), 8)
            hold = hold_rate * stage_f[slot, g * 8:(g + 1) * 8] + stage_s[slot, g * 8:(g + 1) * 8]
            new = latest[r, :] - learn_rate * hold
            latest[r, :] = new
            size = jnp.abs(new)
            most = size[:, :LANES]
            for i in range(1, width // LANES):
                most = jnp.maximum(most, size[:, i * LANES:(i + 1) * LANES])
            part[t, g * 8:(g + 1) * 8] = most

        @pl.when(t + slots < T)
        def _():
            start(t + slots)

    def second_half(side, u):
        latest, ready, base = side[3], side[4], side[6]
        most = part[u]
        for peer in peers:
            @pl.when(u >= quiet)
            def _():
                pltpu.make_async_copy(part_in.at[peer, u], part_in.at[peer, u], part_recv.at[u, peer]).wait()

            most = jnp.maximum(most, part_in[peer, u])
        most = jnp.max(most, axis=1, keepdims=True)
        there = pl.ds(pl.multiple_of((u - base) * K, 16), K)
        scale[pl.ds(pl.multiple_of(u * K, 16), K), :] = jnp.broadcast_to(most, (K, LANES))
        inverse = 1.0 / most
        for g in range(K // 16):
            r = pl.ds(pl.multiple_of((u - base) * K + g * 16, 16), 16)
            ready[r, mine] = (latest[r, :] * inverse[g * 16:(g + 1) * 16]).astype(jnp.bfloat16)
        for i, peer in enumerate(peers):
            pltpu.make_async_remote_copy(
                src_ref=ready.at[there, mine], dst_ref=ready.at[there, mine],
                send_sem=ready_send.at[base // nb, i], recv_sem=ready_recv.at[base // nb, me],
                device_id={"zero": peer}, device_id_type=MESH,
            ).start()

    def columns(side):
        out = side[5]
        for first in range(0, rows, LANES):
            k = min(LANES, rows - first)
            tile = scale[side[6] * K + first:side[6] * K + first + k, :]
            diagonal = lax.broadcasted_iota(jnp.int32, (k, LANES), 0) == lax.broadcasted_iota(jnp.int32, (k, LANES), 1)
            line = jnp.sum(jnp.where(diagonal, tile, 0.0), axis=0)
            out[first:first + k] = line[:k]

    def ahead(t):
        @pl.when(t < nb)
        def _():
            first_half(gate, t)

        @pl.when(t >= nb)
        def _():
            first_half(up, t)

    def behind(u):
        @pl.when(u < nb)
        def _():
            second_half(gate, u)

        @pl.when(u >= nb)
        def _():
            second_half(up, u)

    def send_part(t):
        for i, peer in enumerate(peers):
            pltpu.make_async_remote_copy(
                src_ref=part.at[t], dst_ref=part_in.at[me, t],
                send_sem=part_send.at[i], recv_sem=part_recv.at[t, me],
                device_id={"zero": peer}, device_id_type=MESH,
            ).start()

    def alone(t, carry):
        ahead(t)
        return carry

    def catch_up(i, carry):
        ahead(quiet + i)
        send_part(quiet + i)
        behind(2 * i)
        behind(2 * i + 1)
        return carry

    def steady(t, carry):
        ahead(t)
        send_part(t)
        behind(t - lag)
        return carry

    def last(u, carry):
        behind(u)
        return carry

    lax.fori_loop(0, quiet, alone, 0)
    for c in norm_copies:
        c.wait()
    norm_all[flat, 0, 0:share] = norm_a[...] + norm_b[...]
    norm_all[flat] = pltpu.roll(norm_all[flat], lax.rem(flat * share, LANES), axis=1)
    pl.semaphore_wait(barrier, n - 1)
    early = pl.ds(0, quiet)
    for i, peer in enumerate(peers):
        pltpu.make_async_remote_copy(
            src_ref=part.at[early], dst_ref=part_in.at[me, early],
            send_sem=part_send.at[i], recv_sem=early_recv.at[me],
            device_id={"zero": peer}, device_id_type=MESH,
        ).start()

    def send_norm(d, carry):
        pltpu.make_async_remote_copy(
            src_ref=norm_all.at[flat], dst_ref=norm_all.at[flat],
            send_sem=norm_send, recv_sem=norm_recv,
            device_id=target(d), device_id_type=MESH,
        ).start()
        return carry

    lax.fori_loop(1, n, send_norm, 0)
    for peer in peers:
        pltpu.make_async_copy(part_in.at[peer, early], part_in.at[peer, early], early_recv.at[peer]).wait()
    lax.fori_loop(0, quiet - lag, catch_up, 0)
    lax.fori_loop(2 * quiet - lag, T, steady, 0)
    columns(gate)
    others = norm_all.at[pl.ds(0, n - 1)]
    pltpu.make_async_copy(others, others, norm_send).wait()
    pltpu.make_async_copy(others, others, norm_recv).wait()
    norm_sum[...] = jnp.zeros_like(norm_sum)
    for d in range(n):
        first = d * share // LANES * LANES
        norm_sum[:, first:first + window] += norm_all[d]
    serve_norm[...] = norm_sum[0, :n * share].astype(jnp.bfloat16)
    lax.fori_loop(T - lag, T, last, 0)
    columns(up)

    for i, peer in enumerate(peers):
        pltpu.make_async_copy(part, part, part_send.at[i]).wait()
        theirs = pl.ds(pl.multiple_of(peer * width, LANES), width)
        for half, ready in enumerate((ready_g, ready_u)):
            pltpu.make_async_copy(ready.at[:, mine], ready.at[:, mine], ready_send.at[half, i]).wait()
            pltpu.make_async_copy(ready.at[:, theirs], ready.at[:, theirs], ready_recv.at[half, peer]).wait()


def copy_kernel(*refs):
    count = len(refs) // 2
    sems = refs[-1]
    copies = [pltpu.make_async_copy(refs[i], refs[count + i], sems.at[i]) for i in range(count)]
    for c in copies:
        c.start()
    for c in copies:
        c.wait()


def local(nz, nm, w_gate, first_gate, second_gate, w_up, first_up, second_up, norm_train, norm_step):
    n = nz * nm
    width, rows = w_gate.shape
    share = norm_train.shape[0]
    K = block_rows(rows, 48)
    T = 2 * rows // K
    slots = min(8, T)
    lag = 2
    quiet = max(lag, min(6, (T + lag) // 2))
    window = -(-(share + LANES - 1) // LANES) * LANES
    hbm = pl.BlockSpec(memory_space=pl.ANY)
    vmem = pl.BlockSpec(memory_space=pltpu.VMEM)
    ready_g, ready_u, column_g, column_u, latest_g, latest_u, serve_norm = pl.pallas_call(
        functools.partial(update_kernel, nz, nm, K, slots, lag, quiet),
        out_shape=(
            pltpu.VMEM((rows, nz * width), jnp.bfloat16),
            pltpu.VMEM((rows, nz * width), jnp.bfloat16),
            pltpu.VMEM((rows,), jnp.float32),
            pltpu.VMEM((rows,), jnp.float32),
            pltpu.VMEM((rows, width), jnp.float32),
            pltpu.VMEM((rows, width), jnp.float32),
            pltpu.VMEM((n * share,), jnp.bfloat16),
        ),
        in_specs=[hbm] * 6 + [pl.BlockSpec(memory_space=pltpu.HBM)] * 2,
        out_specs=(vmem,) * 7,
        scratch_shapes=[
            pltpu.VMEM((slots, K, width), jnp.float32),
            pltpu.VMEM((slots, K, width), jnp.float32),
            pltpu.VMEM((T, K, LANES), jnp.float32),
            pltpu.VMEM((nz, T, K, LANES), jnp.float32),
            pltpu.VMEM((2 * rows, LANES), jnp.float32),
            pltpu.VMEM((n, 1, window), jnp.float32),
            pltpu.VMEM((1, n * share + window), jnp.float32),
            pltpu.VMEM((share,), jnp.float32),
            pltpu.VMEM((share,), jnp.float32),
            pltpu.SemaphoreType.DMA((slots,)),
            pltpu.SemaphoreType.DMA((slots,)),
            pltpu.SemaphoreType.DMA((slots,)),
            pltpu.SemaphoreType.DMA((max(nz - 1, 1),)),
            pltpu.SemaphoreType.DMA((T, nz)),
            pltpu.SemaphoreType.DMA((2, max(nz - 1, 1))),
            pltpu.SemaphoreType.DMA((2, nz)),
            pltpu.SemaphoreType.DMA,
            pltpu.SemaphoreType.DMA,
            pltpu.SemaphoreType.DMA((nz,)),
            pltpu.SemaphoreType.DMA((2,)),
        ],
        compiler_params=pltpu.CompilerParams(
            collective_id=0, has_side_effects=True, vmem_limit_bytes=12 * 1024 * 1024
        ),
        name="update",
    )(w_gate.T, first_gate.T, second_gate.T, w_up.T, first_up.T, second_up.T, *(
        pltpu.with_memory_space_constraint(x, pltpu.HBM) for x in (norm_train, norm_step)
    ))
    results = (ready_g, ready_u, column_g, column_u, latest_g, latest_u, serve_norm)
    ready_g, ready_u, column_g, column_u, latest_g, latest_u, serve_norm = pl.pallas_call(
        copy_kernel,
        out_shape=tuple(jax.ShapeDtypeStruct(x.shape, x.dtype) for x in results),
        in_specs=[hbm] * 7,
        out_specs=(hbm,) * 7,
        scratch_shapes=[pltpu.SemaphoreType.DMA((7,))],
        compiler_params=pltpu.CompilerParams(vmem_limit_bytes=1024 * 1024),
        name="write",
    )(*results)
    return (ready_g.T, ready_u.T, column_g, column_u, serve_norm, latest_g.T, latest_u.T)


def solution(mesh):
    whole, both = P("zero", "model"), P(("zero", "model"))
    return jax.shard_map(
        functools.partial(local, mesh.shape["zero"], mesh.shape["model"]),
        mesh=mesh,
        in_specs=(whole,) * 6 + (both,) * 2,
        out_specs=(
            P(None, "model"), P(None, "model"), P("model"), P("model"), P(), whole, whole,
        ),
        check_vma=False,
    )
```
